32 devices in a mesh: groups: 2 (over y), ctx: 8 (over z, x), head: 2 (over core).
Axes of the slice: x: 2, y: 2, z: 4, core: 2. Of those that a mesh axis runs over, the one named last changes fastest.
Arguments:
- query_latent: bfloat16 [16, 64, 576], P(('groups', 'ctx'), 'head'), parts along dimension 0, may hold values from -9 to 9
- latent_codes: bfloat16 [4096, 576], P(('groups', 'ctx')), parts along dimension 0, may hold values from -6 to 6
- latent_scales: float32 [4096, 9], P(('groups', 'ctx')), parts along dimension 0, may hold values from 0.5 to 2
- valid_lengths: int32 [16], P(('groups', 'ctx')), parts along dimension 0, may hold values from 1 to 256
- query_position: int32 [16], P('groups'), parts along dimension 0, may hold values from 0 to 2047
- value_up: bfloat16 [64, 512, 128], P('head'), may hold values from -1 to 1
- out_codes: bfloat16 [8192, 7168], P('head', 'ctx'), may hold values from -0.0625 to 0.0625
- out_scales: float32 [7168], P('ctx'), may hold values from 0.5 to 2
Outputs:
- attention: bfloat16 [16, 8192], P(('groups', 'ctx'), 'head'), parts along dimension 0
- projected: bfloat16 [16, 7168], P(('groups', 'head'), 'ctx'), parts along dimension 0
The draws below stay inside these ranges and needn't reach their ends.
There are 2 independent parts, one for each index of `groups`. The reference program is written for one: setup_inputs(seed, part) draws one part's arguments, and reference() takes and returns one part's arrays. A program takes and returns all parts, laid end to end along the dimension named above; an argument that names none is the same for every part. Nothing has to cross between parts.
All inputs are finite; a program needn't handle non-finite values.
Results may differ from the reference program's by a relative error of at most 0.011.
Values may be sent and summed in bfloat16 or wider, within the bound.
A program may use at most 128 MiB of HBM per device.

```python
import math
import jax
import jax.numpy as jnp
from jax import lax

D = 7168
LAT_NOPE = 512
ROPE = 64
VHEAD = 128
QK_NOPE = 128
HEADS = 64
SBLK = 64
CTX_DEV = 256
LAT = 576
NBLK = 9
CONTEXT = 2048
QTOK = 8
RANKS = 8
N_CTX = 8


def draw_latent_codes(key, part):
    codes = jnp.clip(jax.random.normal(jax.random.fold_in(key, 201), (CONTEXT, LAT), jnp.float32), -6.0, 6.0)
    return codes.astype(jnp.bfloat16)


def draw_query_latent(key, part):
    values = jnp.clip(1.5 * jax.random.normal(jax.random.fold_in(key, 301), (QTOK, HEADS, LAT), jnp.float32), -9.0, 9.0)
    return values.astype(jnp.bfloat16)


def place_ends(entries, own_key, low, top_value):
    longest = entries.shape.index(max(entries.shape))
    spots = []
    for shift in (0, 1):
        where = [jax.random.randint(jax.random.fold_in(own_key, axis), (), 0, length) for axis, length in enumerate(entries.shape)]
        where[longest] = (where[longest] + shift) % entries.shape[longest]
        spots.append(tuple(where))
    return entries.at[spots[0]].set(low).at[spots[1]].set(top_value)


def level_of(key, shape, pieces, smallest, top_value):
    loudness, own = 1.0, jax.random.fold_in(key, 6)
    for dim, shards_of in pieces:
        draws = jnp.exp(jax.random.uniform(jax.random.fold_in(own, dim), (shards_of,), jnp.float32, smallest / len(pieces), top_value / len(pieces)))
        loudness = loudness * jnp.repeat(draws, shape[dim] // shards_of).reshape([-1 if axis == dim else 1 for axis in range(len(shape))])
    return loudness


def gaussian(key, dims, width, reach, split=(), kind=jnp.bfloat16):
    level = level_of(key, dims, split, -0.22, 0.18) if split else 1.0
    drawn = jax.random.normal(key, dims, jnp.float32) * width * level
    return jnp.minimum(jnp.maximum(drawn, -reach), reach).astype(kind)


def setup_inputs(seed: int = 0, part: int = 0) -> dict:
    streams_of = jax.random.split(jax.random.key(seed), 9)
    part_keys = jax.random.split(jax.random.fold_in(streams_of[8], part), 9)
    query_latent = draw_query_latent(jax.random.fold_in(jax.random.fold_in(streams_of[8], part), 71), part)
    latent_codes = draw_latent_codes(jax.random.fold_in(jax.random.fold_in(streams_of[8], part), 71), part)
    latent_scales = jnp.clip(jnp.exp(math.log(2.0) - 1.3862944 * jax.random.uniform(part_keys[2], (CONTEXT, NBLK), jnp.float32) ** level_of(part_keys[2], (CONTEXT, NBLK), ((0, 8),), -0.2, 0.2)), 0.5, 2.0)
    valid_lengths = place_ends(jax.random.randint(part_keys[3], (RANKS,), 1, CTX_DEV + 1), jax.random.fold_in(part_keys[3], 1), 1, CTX_DEV).astype(jnp.int32)
    query_position = place_ends(jax.random.randint(part_keys[4], (QTOK,), 0, CONTEXT), jax.random.fold_in(part_keys[4], 1), 0, CONTEXT - 1).astype(jnp.int32)
    value_up = gaussian(streams_of[5], (HEADS, LAT_NOPE, VHEAD), (LAT_NOPE // 16) ** -0.5, 1.0, ((0, 2),))
    out_codes = gaussian(streams_of[6], (HEADS * VHEAD, D), (HEADS * VHEAD) ** -0.5, 0.0625, ((0, 2), (1, 8)))
    out_scales = jnp.clip(jnp.exp(math.log(2.0) - 1.3862944 * jax.random.uniform(streams_of[7], (D,), jnp.float32) ** level_of(streams_of[7], (D,), ((0, 8),), -0.2, 0.2)), 0.5, 2.0)
    return dict(query_latent=query_latent, latent_codes=latent_codes, latent_scales=latent_scales, valid_lengths=valid_lengths, query_position=query_position, value_up=value_up, out_codes=out_codes, out_scales=out_scales)


def reference(query_latent, latent_codes, latent_scales, valid_lengths, query_position, value_up, out_codes, out_scales):
    latent = (latent_codes.astype(jnp.float32).reshape(CONTEXT, NBLK, SBLK) * latent_scales[:, :, None]).reshape(CONTEXT, LAT).astype(jnp.bfloat16)
    key_pos = jnp.arange(CONTEXT, dtype=jnp.int32)
    owner = key_pos // CTX_DEV
    usable = (key_pos % CTX_DEV) < valid_lengths[owner]
    allowed = usable[None, :] & (key_pos[None, :] <= query_position[:, None])
    softmax_scale = (QK_NOPE + ROPE) ** -0.5
    nope_shards = latent[:, :LAT_NOPE].astype(jnp.float32).reshape(N_CTX, CTX_DEV, LAT_NOPE)

    def one_head(inputs):
        query_head, up_head = inputs
        logits = jnp.dot(query_head, latent.T, preferred_element_type=jnp.float32) * softmax_scale
        logits = jnp.where(allowed, logits, -jnp.inf)
        maxima = jnp.max(logits, axis=1, keepdims=True)
        weights = jnp.exp(logits - maxima)
        totals = jnp.sum(weights, axis=1)
        rounded = lax.optimization_barrier(weights.astype(jnp.bfloat16))
        rounded = rounded.astype(jnp.float32).reshape(QTOK, N_CTX, CTX_DEV)
        partial_mix = lax.optimization_barrier(jnp.einsum("qrk,rkd->rqd", rounded, nope_shards).astype(jnp.bfloat16))
        numerators = jnp.einsum("rqd,dv->qv", partial_mix.astype(jnp.float32), up_head.astype(jnp.float32))
        return numerators / totals[:, None]

    head_outputs = lax.map(one_head, (jnp.transpose(query_latent, (1, 0, 2)), value_up))
    attention = jnp.transpose(head_outputs, (1, 0, 2)).reshape(QTOK, HEADS * VHEAD).astype(jnp.bfloat16)
    projected = (jnp.dot(attention, out_codes, preferred_element_type=jnp.float32) * out_scales[None, :]).astype(jnp.bfloat16)
    return attention, projected
```

```python
import functools

import jax
import jax.numpy as jnp
from jax import lax
from jax.experimental import pallas as pl
from jax.experimental.pallas import tpu as pltpu
from jax.sharding import PartitionSpec as P

LAT_NOPE = 512
ROPE = 64
QK_NOPE = 128
LANES = 128
MASKED = -1e30
MESH = pl.DeviceIdType.MESH


def shards(
    query_latent,
    latent_codes,
    latent_scales,
    valid_lengths,
    query_position,
    value_up,
    out_codes,
    out_scales,
):
    key_count, width = latent_codes.shape
    block_count = latent_scales.shape[1]
    latent = (
        (
            latent_codes.astype(jnp.float32).reshape(key_count, block_count, width // block_count)
            * latent_scales[:, :, None]
        )
        .reshape(key_count, width)
        .astype(jnp.bfloat16)
    )
    shard_index = lax.axis_index("ctx")
    local_slots = jnp.arange(key_count, dtype=jnp.int32)
    key_pos = shard_index * key_count + local_slots
    usable = local_slots < valid_lengths[0]
    softmax_scale = (QK_NOPE + ROPE) ** (-0.5)
    logits = (
        jnp.einsum(
            "qhc,kc->qhk",
            lax.all_gather(query_latent, "ctx", axis=0, tiled=True),
            latent,
            preferred_element_type=jnp.float32,
        )
        * softmax_scale
    )
    allowed = usable[None, :] & (key_pos[None, :] <= query_position[:, None])
    scores = jnp.where(allowed[:, None, :], logits, -jnp.inf)
    maxima = lax.pmax(jnp.max(scores, axis=2), "ctx")
    weights = jnp.exp(scores - maxima[:, :, None])
    totals = jnp.sum(weights, axis=2)
    latent_mix = jnp.einsum(
        "qhk,kd->qhd",
        weights.astype(jnp.bfloat16),
        latent[:, :LAT_NOPE],
        preferred_element_type=jnp.float32,
    ).astype(jnp.bfloat16)
    values = jnp.einsum("qhd,hdv->qhv", latent_mix, value_up, preferred_element_type=jnp.float32)
    queries, head_count, value_width = values.shape
    numerators = values.reshape(queries, head_count * value_width)
    own_rows = query_latent.shape[0]
    numer_sum, denom_sum = lax.psum((numerators, totals), "ctx")
    attn_all = (
        (numer_sum.reshape(queries, head_count, value_width) / denom_sum[:, :, None])
        .reshape(queries, head_count * value_width)
        .astype(jnp.bfloat16)
    )
    attn_home = lax.dynamic_slice_in_dim(attn_all, shard_index * own_rows, own_rows, 0)
    summed = lax.psum_scatter(
        jnp.dot(attn_all, out_codes, preferred_element_type=jnp.float32),
        "head",
        scatter_dimension=0,
        tiled=True,
    )
    projected = (summed * out_scales[None, :]).astype(jnp.bfloat16)
    return (attn_home, projected)


def fused(
    n,
    heads,
    valid_ref,
    qpos_ref,
    query_hbm,
    codes_hbm,
    scales_hbm,
    up_hbm,
    out_hbm,
    out_scales_ref,
    attn_ref,
    proj_ref,
    q_all,
    codes,
    scales,
    up,
    outw,
    latent,
    mix,
    stat_m,
    stat_l,
    num_send,
    num_recv,
    st_send,
    st_recv,
    att_all,
    part,
    part_recv,
    in_sem,
    up_sem,
    out_sem,
    q_send,
    q_recv,
    num_ssem,
    num_rsem,
    st_ssem,
    st_rsem,
    att_ssem,
    att_rsem,
    part_ssem,
    part_rsem,
):
    me = lax.axis_index("ctx")
    hd = lax.axis_index("head")
    side = lax.rem(me, 2)
    partner = me + 1 - 2 * side
    half = n // 2
    tokens, head_count, width = q_all.shape
    keys = codes.shape[0]
    nope = mix.shape[0] * LANES
    vhead = up.shape[2]
    per = head_count // n
    cols = per * vhead

    def at(k):
        return lax.rem(me + k + n, n)

    barrier = pltpu.get_barrier_semaphore()
    for k in range(1, n):
        pl.semaphore_signal(barrier, inc=1, device_id={"ctx": at(k)}, device_id_type=MESH)
    for k in range(1, heads):
        pl.semaphore_signal(
            barrier, inc=1, device_id={"head": lax.rem(hd + k, heads)}, device_id_type=MESH
        )

    own_q = pltpu.make_async_copy(query_hbm.at[0], q_all.at[me], in_sem.at[0])
    own_q.start()
    codes_in = pltpu.make_async_copy(codes_hbm, codes, in_sem.at[1])
    codes_in.start()
    scales_in = pltpu.make_async_copy(scales_hbm, scales, in_sem.at[2])
    scales_in.start()
    up_in = []
    for g in range(n):
        rows = pl.ds(g * per, per)
        up_in.append(pltpu.make_async_copy(up_hbm.at[rows], up.at[rows], up_sem.at[g]))
        up_in[-1].start()
    out_in = []
    for g in range(n):
        rows = pl.ds(g * cols, cols)
        out_in.append(pltpu.make_async_copy(out_hbm.at[rows], outw.at[rows], out_sem.at[g]))
        out_in[-1].start()

    own_q.wait()
    pl.semaphore_wait(barrier, n - 1 + heads - 1)

    def send_q(token, target, index):
        copy = pltpu.make_async_remote_copy(
            src_ref=q_all.at[token],
            dst_ref=q_all.at[token],
            send_sem=q_send.at[index],
            recv_sem=q_recv.at[index],
            device_id={"ctx": target},
            device_id_type=MESH,
        )
        copy.start()
        return copy

    sent = [send_q(me, partner, half)]
    direct = [send_q(me, at(2 * k), k) for k in range(1, half)]

    codes_in.wait()
    scales_in.wait()
    block = width // scales.shape[1]
    lane = lax.broadcasted_iota(jnp.int32, (keys, LANES), 1)
    for start in range(0, width, LANES):
        span = min(LANES, width - start)
        first = start // block
        scale = jnp.broadcast_to(scales[:, first : first + 1], (keys, LANES))
        for b in range(1, span // block):
            scale = jnp.where(lane >= b * block, scales[:, first + b : first + b + 1], scale)
        latent[:, start : start + span] = (
            codes[:, start : start + span].astype(jnp.float32) * scale[:, :span]
        ).astype(jnp.bfloat16)

    for k in range(1, half):
        direct[k - 1].wait_recv()
        sent.append(send_q(at(-2 * k), partner, half + k))
    for copy in sent:
        copy.wait_recv()

    softmax_scale = (QK_NOPE + ROPE) ** (-0.5)
    logits = (
        lax.dot_general(
            q_all[...].reshape(tokens * head_count, width),
            latent[...],
            (((1,), (1,)), ((), ())),
            preferred_element_type=jnp.float32,
        )
        * softmax_scale
    )
    slot = lax.broadcasted_iota(jnp.int32, (head_count, keys), 1)
    weights = []
    for t in range(tokens):
        limit = jnp.minimum(valid_ref[0], qpos_ref[t] - me * keys + 1)
        allowed = slot < limit
        rows = slice(t * head_count, (t + 1) * head_count)
        scores = jnp.where(allowed, logits[rows], MASKED)
        top = jnp.max(scores, axis=1, keepdims=True)
        weight = jnp.where(allowed, jnp.exp(scores - top), 0.0)
        stat_m[rows, :] = jnp.broadcast_to(top, (head_count, LANES))
        stat_l[rows, :] = jnp.broadcast_to(jnp.sum(weight, axis=1, keepdims=True), (head_count, LANES))
        weights.append(weight.astype(jnp.bfloat16))
    mixed_all = jnp.dot(
        jnp.concatenate(weights, axis=0), latent[:, :nope], preferred_element_type=jnp.float32
    )
    for c in range(mix.shape[0]):
        mix[c] = mixed_all[:, c * LANES : (c + 1) * LANES]

    tile_lane = lax.broadcasted_iota(jnp.int32, (tokens, LANES), 1)
    for g in range(n):
        up_in[g].wait()
        stat = jnp.zeros((tokens, LANES), jnp.float32)
        for j in range(per):
            h = g * per + j
            rows = pl.ds(h, tokens, stride=head_count)
            mixed = jnp.concatenate(
                [mix[c, rows, :] for c in range(mix.shape[0])], axis=1
            ).astype(jnp.bfloat16)
            num_send[g, :, j * vhead : (j + 1) * vhead] = jnp.dot(
                mixed, up[h], preferred_element_type=jnp.float32
            ).astype(jnp.bfloat16)
            stat = jnp.where(tile_lane == j, stat_m[rows, :], stat)
            stat = jnp.where(tile_lane == per + j, stat_l[rows, :], stat)
        st_send[g] = stat

    moved = []
    for k in range(1, n):
        target = at(k)
        for src, dst, ssem, rsem in (
            (st_send, st_recv, st_ssem, st_rsem),
            (num_send, num_recv, num_ssem, num_rsem),
        ):
            copy = pltpu.make_async_remote_copy(
                src_ref=src.at[target],
                dst_ref=dst.at[k],
                send_sem=ssem.at[k],
                recv_sem=rsem.at[k],
                device_id={"ctx": target},
                device_id_type=MESH,
            )
            copy.start()
            moved.append(copy)
    for copy in direct + sent:
        copy.wait_send()
    for copy in moved:
        copy.wait_recv()

    stats = [st_send[me]] + [st_recv[k] for k in range(1, n)]
    nums = [num_send[me]] + [num_recv[k] for k in range(1, n)]
    top = functools.reduce(jnp.maximum, stats)
    factors = [jnp.exp(s - top) for s in stats]
    pieces = []
    for j in range(per):
        total = jnp.zeros((tokens, 1), jnp.float32)
        value = jnp.zeros((tokens, vhead), jnp.float32)
        for s, f, v in zip(stats, factors, nums):
            factor = f[:, j : j + 1]
            total += factor * s[:, per + j : per + j + 1]
            value += factor * v[:, j * vhead : (j + 1) * vhead].astype(jnp.float32)
        pieces.append((value / total).astype(jnp.bfloat16))
    att_all[me] = jnp.concatenate(pieces, axis=1)

    shared = []
    for k in range(1, n):
        copy = pltpu.make_async_remote_copy(
            src_ref=att_all.at[me],
            dst_ref=att_all.at[me],
            send_sem=att_ssem.at[k],
            recv_sem=att_rsem.at[k],
            device_id={"ctx": at(k)},
            device_id_type=MESH,
        )
        copy.start()
        shared.append(copy)
    for copy in moved:
        copy.wait_send()
    for copy in out_in:
        copy.wait()
    columns = outw.shape[1]
    acc = jnp.zeros((tokens, columns), jnp.float32)
    for k in range(n):
        if k:
            shared[k - 1].wait_recv()
        g = at(-k)
        acc += jnp.dot(
            att_all[g],
            outw[pl.ds(pl.multiple_of(g * cols, cols), cols), :],
            preferred_element_type=jnp.float32,
        )
    rows = tokens // heads
    for i in range(heads):
        part[i] = acc[i * rows : (i + 1) * rows]
    swapped = []
    for k in range(1, heads):
        other = lax.rem(hd + k, heads)
        copy = pltpu.make_async_remote_copy(
            src_ref=part.at[other],
            dst_ref=part_recv.at[k],
            send_sem=part_ssem.at[k],
            recv_sem=part_rsem.at[k],
            device_id={"head": other},
            device_id_type=MESH,
        )
        copy.start()
        swapped.append(copy)
    row = lax.broadcasted_iota(jnp.int32, (tokens, cols), 0)
    for g in range(n):
        attn_ref[:, g * cols : (g + 1) * cols] = jnp.sum(
            jnp.where(row == me, att_all[g].astype(jnp.float32), 0.0), axis=0, keepdims=True
        ).astype(jnp.bfloat16)
    summed = part[hd]
    for k in range(1, heads):
        swapped[k - 1].wait_recv()
        summed += part_recv[k]
    proj_ref[...] = (summed * out_scales_ref[...]).astype(jnp.bfloat16)
    for copy in shared + swapped:
        copy.wait_send()


def block(n, heads, *args):
    query, codes, scales, valid, qpos, up, outw, out_scales = args
    own, head_count, width = query.shape
    tokens = own * n
    fits = own == 1 and n % 2 == 0 and head_count % n == 0 and tokens % (4 * heads) == 0
    if not fits:
        return shards(*args)
    keys = codes.shape[0]
    vhead = up.shape[2]
    per = head_count // n
    cols = per * vhead
    columns = outw.shape[1]
    anywhere = pl.BlockSpec(memory_space=pl.ANY)
    vmem = pl.BlockSpec(memory_space=pltpu.VMEM)
    smem = pl.BlockSpec(memory_space=pltpu.SMEM)
    dma = pltpu.SemaphoreType.DMA
    return pl.pallas_call(
        functools.partial(fused, n, heads),
        out_shape=(
            jax.ShapeDtypeStruct((own, head_count * vhead), jnp.bfloat16),
            jax.ShapeDtypeStruct((tokens // heads, columns), jnp.bfloat16),
        ),
        in_specs=[smem, smem] + [anywhere] * 5 + [vmem],
        out_specs=(vmem, vmem),
        scratch_shapes=[
            pltpu.VMEM((tokens, head_count, width), jnp.bfloat16),
            pltpu.VMEM(codes.shape, jnp.bfloat16),
            pltpu.VMEM(scales.shape, jnp.float32),
            pltpu.VMEM(up.shape, jnp.bfloat16),
            pltpu.VMEM(outw.shape, jnp.bfloat16),
            pltpu.VMEM((keys, width), jnp.bfloat16),
            pltpu.VMEM((LAT_NOPE // LANES, tokens * head_count, LANES), jnp.float32),
            pltpu.VMEM((tokens * head_count, LANES), jnp.float32),
            pltpu.VMEM((tokens * head_count, LANES), jnp.float32),
            pltpu.VMEM((n, tokens, cols), jnp.bfloat16),
            pltpu.VMEM((n, tokens, cols), jnp.bfloat16),
            pltpu.VMEM((n, tokens, LANES), jnp.float32),
            pltpu.VMEM((n, tokens, LANES), jnp.float32),
            pltpu.VMEM((n, tokens, cols), jnp.bfloat16),
            pltpu.VMEM((heads, tokens // heads, columns), jnp.float32),
            pltpu.VMEM((heads, tokens // heads, columns), jnp.float32),
            dma((3,)),
            dma((n,)),
            dma((n,)),
            dma((n,)),
            dma((n,)),
            dma((n,)),
            dma((n,)),
            dma((n,)),
            dma((n,)),
            dma((n,)),
            dma((n,)),
            dma((heads,)),
            dma((heads,)),
        ],
        compiler_params=pltpu.CompilerParams(collective_id=0, has_side_effects=True),
        name="mla_block",
    )(valid, qpos, query, codes, scales, up, outw, out_scales.reshape(1, -1))


def solution(mesh):
    ctx, heads = mesh.shape["ctx"], mesh.shape["head"]
    return jax.shard_map(
        functools.partial(block, ctx, heads),
        mesh=mesh,
        in_specs=(
            P(("groups", "ctx"), "head", None),
            P(("groups", "ctx"), None),
            P(("groups", "ctx"), None),
            P(("groups", "ctx")),
            P("groups"),
            P("head", None, None),
            P("head", "ctx"),
            P("ctx"),
        ),
        out_specs=(P(("groups", "ctx"), "head"), P(("groups", "head"), "ctx")),
        check_vma=False,
    )
```

```python
import functools

import jax
import jax.numpy as jnp
from jax import lax
from jax.experimental import pallas as pl
from jax.experimental.pallas import tpu as pltpu
from jax.sharding import PartitionSpec as P

LAT_NOPE = 512
ROPE = 64
QK_NOPE = 128
LANES = 128
MASKED = -1e30
MESH = pl.DeviceIdType.MESH


def shards(
    query_latent,
    latent_codes,
    latent_scales,
    valid_lengths,
    query_position,
    value_up,
    out_codes,
    out_scales,
):
    key_count, width = latent_codes.shape
    block_count = latent_scales.shape[1]
    latent = (
        (
            latent_codes.astype(jnp.float32).reshape(key_count, block_count, width // block_count)
            * latent_scales[:, :, None]
        )
        .reshape(key_count, width)
        .astype(jnp.bfloat16)
    )
    shard_index = lax.axis_index("ctx")
    local_slots = jnp.arange(key_count, dtype=jnp.int32)
    key_pos = shard_index * key_count + local_slots
    usable = local_slots < valid_lengths[0]
    softmax_scale = (QK_NOPE + ROPE) ** (-0.5)
    logits = (
        jnp.einsum(
            "qhc,kc->qhk",
            lax.all_gather(query_latent, "ctx", axis=0, tiled=True),
            latent,
            preferred_element_type=jnp.float32,
        )
        * softmax_scale
    )
    allowed = usable[None, :] & (key_pos[None, :] <= query_position[:, None])
    scores = jnp.where(allowed[:, None, :], logits, -jnp.inf)
    maxima = lax.pmax(jnp.max(scores, axis=2), "ctx")
    weights = jnp.exp(scores - maxima[:, :, None])
    totals = jnp.sum(weights, axis=2)
    latent_mix = jnp.einsum(
        "qhk,kd->qhd",
        weights.astype(jnp.bfloat16),
        latent[:, :LAT_NOPE],
        preferred_element_type=jnp.float32,
    ).astype(jnp.bfloat16)
    values = jnp.einsum("qhd,hdv->qhv", latent_mix, value_up, preferred_element_type=jnp.float32)
    queries, head_count, value_width = values.shape
    numerators = values.reshape(queries, head_count * value_width)
    own_rows = query_latent.shape[0]
    numer_sum, denom_sum = lax.psum((numerators, totals), "ctx")
    attn_all = (
        (numer_sum.reshape(queries, head_count, value_width) / denom_sum[:, :, None])
        .reshape(queries, head_count * value_width)
        .astype(jnp.bfloat16)
    )
    attn_home = lax.dynamic_slice_in_dim(attn_all, shard_index * own_rows, own_rows, 0)
    summed = lax.psum_scatter(
        jnp.dot(attn_all, out_codes, preferred_element_type=jnp.float32),
        "head",
        scatter_dimension=0,
        tiled=True,
    )
    projected = (summed * out_scales[None, :]).astype(jnp.bfloat16)
    return (attn_home, projected)


def fused(
    n,
    heads,
    valid_ref,
    qpos_ref,
    query_hbm,
    codes_hbm,
    scales_hbm,
    up_hbm,
    out_hbm,
    attn_ref,
    proj_ref,
    q_all,
    codes,
    scales,
    up,
    outw,
    latent,
    mix,
    stat_m,
    stat_l,
    num_send,
    num_recv,
    st_send,
    st_recv,
    att_all,
    part,
    part_recv,
    in_sem,
    up_sem,
    out_sem,
    q_send,
    q_recv,
    num_ssem,
    num_rsem,
    st_ssem,
    st_rsem,
    att_ssem,
    att_rsem,
    part_ssem,
    part_rsem,
):
    me = lax.axis_index("ctx")
    hd = lax.axis_index("head")
    side = lax.rem(me, 2)
    partner = me + 1 - 2 * side
    half = n // 2
    tokens, head_count, width = q_all.shape
    keys = codes.shape[1]
    nope = mix.shape[0] * LANES
    vhead = up.shape[2]
    per = head_count // n
    cols = per * vhead

    def at(k):
        return lax.rem(me + k + n, n)

    barrier = pltpu.get_barrier_semaphore()
    for k in range(1, n):
        pl.semaphore_signal(barrier, inc=1, device_id={"ctx": at(k)}, device_id_type=MESH)
    for k in range(1, heads):
        pl.semaphore_signal(
            barrier, inc=1, device_id={"head": lax.rem(hd + k, heads)}, device_id_type=MESH
        )

    own_q = pltpu.make_async_copy(query_hbm.at[0], q_all.at[me], in_sem.at[0])
    own_q.start()
    codes_in = pltpu.make_async_copy(codes_hbm, codes, in_sem.at[1])
    codes_in.start()
    scales_in = pltpu.make_async_copy(scales_hbm, scales, in_sem.at[2])
    scales_in.start()
    up_in = []
    for g in range(n):
        rows = pl.ds(g * per, per)
        up_in.append(pltpu.make_async_copy(up_hbm.at[rows], up.at[rows], up_sem.at[g]))
        up_in[-1].start()
    out_in = []
    for g in range(n):
        rows = pl.ds(g * cols, cols)
        out_in.append(pltpu.make_async_copy(out_hbm.at[rows], outw.at[rows], out_sem.at[g]))
        out_in[-1].start()

    own_q.wait()
    pl.semaphore_wait(barrier, n - 1 + heads - 1)

    def send_q(token, target, index):
        copy = pltpu.make_async_remote_copy(
            src_ref=q_all.at[token],
            dst_ref=q_all.at[token],
            send_sem=q_send.at[index],
            recv_sem=q_recv.at[index],
            device_id={"ctx": target},
            device_id_type=MESH,
        )
        copy.start()
        return copy

    sent = [send_q(me, partner, half)]
    direct = [send_q(me, at(2 * k), k) for k in range(1, half)]

    codes_in.wait()
    scales_in.wait()
    block = width // scales.shape[0]
    for b in range(scales.shape[0]):
        rows = slice(b * block, (b + 1) * block)
        latent[rows, :] = (codes[rows, :].astype(jnp.float32) * scales[b : b + 1, :]).astype(jnp.bfloat16)

    for k in range(1, half):
        direct[k - 1].wait_recv()
        sent.append(send_q(at(-2 * k), partner, half + k))
    for copy in sent:
        copy.wait_recv()

    softmax_scale = (QK_NOPE + ROPE) ** (-0.5)
    logits = (
        jnp.dot(
            q_all[...].reshape(tokens * head_count, width),
            latent[...],
            preferred_element_type=jnp.float32,
        )
        * softmax_scale
    )
    slot = lax.broadcasted_iota(jnp.int32, (head_count, keys), 1)
    weights = []
    for t in range(tokens):
        limit = jnp.minimum(valid_ref[0], qpos_ref[t] - me * keys + 1)
        allowed = slot < limit
        rows = slice(t * head_count, (t + 1) * head_count)
        scores = jnp.where(allowed, logits[rows], MASKED)
        top = jnp.max(scores, axis=1, keepdims=True)
        weight = jnp.where(allowed, jnp.exp(scores - top), 0.0)
        stat_m[rows, :] = jnp.broadcast_to(top, (head_count, LANES))
        stat_l[rows, :] = jnp.broadcast_to(jnp.sum(weight, axis=1, keepdims=True), (head_count, LANES))
        weights.append(weight.astype(jnp.bfloat16))
    mixed_all = lax.dot_general(
        jnp.concatenate(weights, axis=0),
        latent[:nope, :],
        (((1,), (1,)), ((), ())),
        preferred_element_type=jnp.float32,
    )
    for c in range(mix.shape[0]):
        mix[c] = mixed_all[:, c * LANES : (c + 1) * LANES]

    tile_lane = lax.broadcasted_iota(jnp.int32, (tokens, LANES), 1)
    for g in range(n):
        up_in[g].wait()
        stat = jnp.zeros((tokens, LANES), jnp.float32)
        for j in range(per):
            h = g * per + j
            rows = pl.ds(h, tokens, stride=head_count)
            mixed = jnp.concatenate(
                [mix[c, rows, :] for c in range(mix.shape[0])], axis=1
            ).astype(jnp.bfloat16)
            num_send[g, :, j * vhead : (j + 1) * vhead] = jnp.dot(
                mixed, up[h], preferred_element_type=jnp.float32
            ).astype(jnp.bfloat16)
            stat = jnp.where(tile_lane == j, stat_m[rows, :], stat)
            stat = jnp.where(tile_lane == per + j, stat_l[rows, :], stat)
        st_send[g] = stat

    moved = []
    for k in range(1, n):
        target = at(k)
        for src, dst, ssem, rsem in (
            (st_send, st_recv, st_ssem, st_rsem),
            (num_send, num_recv, num_ssem, num_rsem),
        ):
            copy = pltpu.make_async_remote_copy(
                src_ref=src.at[target],
                dst_ref=dst.at[k],
                send_sem=ssem.at[k],
                recv_sem=rsem.at[k],
                device_id={"ctx": target},
                device_id_type=MESH,
            )
            copy.start()
            moved.append(copy)
    for copy in direct + sent:
        copy.wait_send()
    for copy in moved:
        copy.wait_recv()

    stats = [st_send[me]] + [st_recv[k] for k in range(1, n)]
    nums = [num_send[me]] + [num_recv[k] for k in range(1, n)]
    top = functools.reduce(jnp.maximum, stats)
    factors = [jnp.exp(s - top) for s in stats]
    pieces = []
    for j in range(per):
        total = jnp.zeros((tokens, 1), jnp.float32)
        value = jnp.zeros((tokens, vhead), jnp.float32)
        for s, f, v in zip(stats, factors, nums):
            factor = f[:, j : j + 1]
            total += factor * s[:, per + j : per + j + 1]
            value += factor * v[:, j * vhead : (j + 1) * vhead].astype(jnp.float32)
        pieces.append((value / total).astype(jnp.bfloat16))
    att_all[me] = jnp.concatenate(pieces, axis=1)

    shared = []
    for k in range(1, n):
        copy = pltpu.make_async_remote_copy(
            src_ref=att_all.at[me],
            dst_ref=att_all.at[me],
            send_sem=att_ssem.at[k],
            recv_sem=att_rsem.at[k],
            device_id={"ctx": at(k)},
            device_id_type=MESH,
        )
        copy.start()
        shared.append(copy)
    for copy in moved:
        copy.wait_send()
    for copy in out_in:
        copy.wait()
    columns = outw.shape[1]
    acc = jnp.zeros((tokens, columns), jnp.float32)
    for k in range(n):
        if k:
            shared[k - 1].wait_recv()
        g = at(-k)
        acc += jnp.dot(
            att_all[g],
            outw[pl.ds(pl.multiple_of(g * cols, cols), cols), :],
            preferred_element_type=jnp.float32,
        )
    rows = tokens // heads
    for i in range(heads):
        part[i] = acc[i * rows : (i + 1) * rows]
    swapped = []
    for k in range(1, heads):
        other = lax.rem(hd + k, heads)
        copy = pltpu.make_async_remote_copy(
            src_ref=part.at[other],
            dst_ref=part_recv.at[k],
            send_sem=part_ssem.at[k],
            recv_sem=part_rsem.at[k],
            device_id={"head": other},
            device_id_type=MESH,
        )
        copy.start()
        swapped.append(copy)
    row = lax.broadcasted_iota(jnp.int32, (tokens, cols), 0)
    for g in range(n):
        attn_ref[:, g * cols : (g + 1) * cols] = jnp.sum(
            jnp.where(row == me, att_all[g].astype(jnp.float32), 0.0), axis=0, keepdims=True
        )
    summed = part[hd]
    for k in range(1, heads):
        swapped[k - 1].wait_recv()
        summed += part_recv[k]
    proj_ref[...] = summed
    for copy in shared + swapped:
        copy.wait_send()


def block(n, heads, *args):
    query, codes, scales, valid, qpos, up, outw, out_scales = args
    own, head_count, width = query.shape
    tokens = own * n
    fits = own == 1 and n % 2 == 0 and head_count % n == 0 and tokens % (4 * heads) == 0
    if not fits:
        return shards(*args)
    keys = codes.shape[0]
    vhead = up.shape[2]
    per = head_count // n
    cols = per * vhead
    columns = outw.shape[1]
    anywhere = pl.BlockSpec(memory_space=pl.ANY)
    vmem = pl.BlockSpec(memory_space=pltpu.VMEM)
    smem = pl.BlockSpec(memory_space=pltpu.SMEM)
    dma = pltpu.SemaphoreType.DMA
    attention, summed = pl.pallas_call(
        functools.partial(fused, n, heads),
        out_shape=(
            jax.ShapeDtypeStruct((own, head_count * vhead), jnp.float32),
            jax.ShapeDtypeStruct((tokens // heads, columns), jnp.float32),
        ),
        in_specs=[smem, smem] + [anywhere] * 5,
        out_specs=(vmem, vmem),
        scratch_shapes=[
            pltpu.VMEM((tokens, head_count, width), jnp.bfloat16),
            pltpu.VMEM((width, keys), jnp.bfloat16),
            pltpu.VMEM(scales.shape[::-1], jnp.float32),
            pltpu.VMEM(up.shape, jnp.bfloat16),
            pltpu.VMEM(outw.shape, jnp.bfloat16),
            pltpu.VMEM((width, keys), jnp.bfloat16),
            pltpu.VMEM((LAT_NOPE // LANES, tokens * head_count, LANES), jnp.float32),
            pltpu.VMEM((tokens * head_count, LANES), jnp.float32),
            pltpu.VMEM((tokens * head_count, LANES), jnp.float32),
            pltpu.VMEM((n, tokens, cols), jnp.bfloat16),
            pltpu.VMEM((n, tokens, cols), jnp.bfloat16),
            pltpu.VMEM((n, tokens, LANES), jnp.float32),
            pltpu.VMEM((n, tokens, LANES), jnp.float32),
            pltpu.VMEM((n, tokens, cols), jnp.bfloat16),
            pltpu.VMEM((heads, tokens // heads, columns), jnp.float32),
            pltpu.VMEM((heads, tokens // heads, columns), jnp.float32),
            dma((3,)),
            dma((n,)),
            dma((n,)),
            dma((n,)),
            dma((n,)),
            dma((n,)),
            dma((n,)),
            dma((n,)),
            dma((n,)),
            dma((n,)),
            dma((n,)),
            dma((heads,)),
            dma((heads,)),
        ],
        compiler_params=pltpu.CompilerParams(collective_id=0, has_side_effects=True),
        name="mla_block",
    )(valid, qpos, query, codes.T, scales.T, up, outw)
    projected = (summed * out_scales[None, :]).astype(jnp.bfloat16)
    return attention.astype(jnp.bfloat16), projected


def solution(mesh):
    ctx, heads = mesh.shape["ctx"], mesh.shape["head"]
    return jax.shard_map(
        functools.partial(block, ctx, heads),
        mesh=mesh,
        in_specs=(
            P(("groups", "ctx"), "head", None),
            P(("groups", "ctx"), None),
            P(("groups", "ctx"), None),
            P(("groups", "ctx")),
            P("groups"),
            P("head", None, None),
            P("head", "ctx"),
            P("ctx"),
        ),
        out_specs=(P(("groups", "ctx"), "head"), P(("groups", "head"), "ctx")),
        check_vma=False,
    )
```
